32 devices in a mesh: groups: 1, tensor: 32 (over z, y, x, core).
Axes of the slice: x: 2, y: 2, z: 4, core: 2. Of those that a mesh axis runs over, the one named last changes fastest.
Arguments:
- hidden_in: bfloat16 [4, 16384], P('groups', 'tensor'), may hold values from -0.59765625 to 0.59765625
- norm_gain: bfloat16 [16384], P('tensor'), may hold values from 0.5 to 1.5
- w_q: bfloat16 [16384, 16384], P('tensor'), may hold values from -1 to 256
- w_kv: bfloat16 [16384, 2048], P('tensor'), may hold values from -0.046875 to 0.046875
- w_o: bfloat16 [16384, 16384], P(None, 'tensor'), may hold values from -0.046875 to 0.046875
- kv_cache: bfloat16 [8, 4, 2, 4096, 128], P(None, 'groups', None, 'tensor'), may hold values from -8 to 8
- lengths: int32 [4], P('groups'), may hold values from 2 to 4096, as said below
- slab_index: int32 [8, 4], P(None, 'groups'), may hold values from 0 to 3, each once within a row
Outputs:
- hidden_out: bfloat16 [4, 16384], P('groups', 'tensor')
The draws below stay inside these ranges and needn't reach their ends.
Inputs may be any that keep to these rules, and one draw needn't show every extreme that they name: `lengths`: one request in every draw has exactly 4096 cached tokens.
All inputs are finite; a program needn't handle non-finite values.
Results may differ from the reference program's by a relative error of at most 0.0085.
The reference program's roundings to bfloat16 on the way count: a program that leaves them out, or rounds other values in their place, can miss the bound.
Values may be sent and summed in bfloat16 or wider, within the bound.
A program may use at most 128 MiB of HBM per device.

```python
import jax
import jax.numpy as jnp
from jax import lax

KVH = 8
HD = 128
GROUP = 16
D = 16384
CTX = 4096
BATCH = 4


def draw_lengths(key, part):
    picked = jax.random.randint(jax.random.fold_in(key, 11), (BATCH,), 2, CTX + 1)
    longest = jax.random.randint(jax.random.fold_in(key, 12), (), 0, BATCH)
    return jnp.where(jnp.arange(BATCH) == longest, CTX, picked).astype(jnp.int32)


def draw_w_q(key, part):
    weight_scale = D ** (-0.5)
    base = jax.random.normal(jax.random.fold_in(key, 31), (D, D), jnp.float32) * weight_scale
    base = jnp.clip(base, -6.0 * weight_scale, 6.0 * weight_scale)
    return base.astype(jnp.bfloat16)


def draw_kv_cache(key, part):
    base = 2.0 * jax.random.normal(jax.random.fold_in(key, 21), (KVH, BATCH, 2, CTX, HD), jnp.float32)
    return jnp.clip(base, -8.0, 8.0).astype(jnp.bfloat16)


def block_levels(rng, dims, shards, smallest, largest):
    level = 1.0
    for axis_at, blocks in shards:
        heights = jax.random.uniform(jax.random.fold_in(jax.random.fold_in(rng, 6), axis_at), (blocks,), jnp.float32, smallest / len(shards), largest / len(shards))
        level = level * jnp.repeat(jnp.exp(heights), dims[axis_at] // blocks).reshape((-1,) + (1,) * (len(dims) - 1 - axis_at))
    return level


def noise(rng, dims, width, reach, pieces=(), held_as=jnp.bfloat16):
    gain = block_levels(rng, dims, pieces, -0.22, 0.18) if pieces else 1.0
    values = jax.random.normal(rng, dims, jnp.float32) * width * gain
    return jnp.minimum(jnp.maximum(values, -reach), reach).astype(held_as)


def setup_inputs(seed: int = 0, part: int = 0) -> dict:
    key_of = jax.random.split(jax.random.key(seed), 9)
    own_keys = jax.random.split(jax.random.fold_in(key_of[8], part), 9)
    return {
        "hidden_in": noise(own_keys[0], (BATCH, D), 0.1, 0.59765625, ((1, 32),)),
        "norm_gain": jnp.clip(1.0 + 0.1 * jax.random.normal(key_of[1], (D,), jnp.float32), 0.5, 1.5).astype(jnp.bfloat16),
        "w_q": draw_w_q(jax.random.fold_in(key_of[8], 71), part),
        "w_kv": noise(key_of[3], (D, 2 * KVH * HD), D ** -0.5, 0.046875, ((0, 32),)),
        "w_o": noise(key_of[4], (D, D), D ** -0.5, 0.046875, ((1, 32),)),
        "kv_cache": draw_kv_cache(jax.random.fold_in(jax.random.fold_in(key_of[8], part), 71), part),
        "lengths": draw_lengths(jax.random.fold_in(jax.random.fold_in(key_of[8], part), 71), part),
        "slab_index": jax.vmap(lambda own: jax.random.permutation(own, BATCH))(jax.random.split(own_keys[7], KVH)).reshape((KVH, BATCH)).astype(jnp.int32),
    }


epsilon = 1e-05
rope_base = 500000.0

def rotate(values, position):
    head_dim = values.shape[-1]
    half_dim = head_dim // 2
    frequency = rope_base ** (-2.0 * jnp.arange(half_dim, dtype=jnp.float32) / head_dim)
    angles = position[..., None] * frequency
    cosine = jnp.cos(angles)
    sines = jnp.sin(angles)
    lower_half = values[..., :half_dim]
    upper_half = values[..., half_dim:]
    return jnp.concatenate([lower_half * cosine - upper_half * sines, upper_half * cosine + lower_half * sines], axis=-1)

def reference(hidden_in, norm_gain, w_q, w_kv, w_o, kv_cache, lengths, slab_index):
    stream = hidden_in.astype(jnp.float32)
    squares = lax.optimization_barrier(jnp.mean(stream * stream, axis=1, keepdims=True))
    normed = (stream * lax.rsqrt(squares + epsilon) * norm_gain.astype(jnp.float32)).astype(jnp.bfloat16)
    proj_q = jnp.dot(normed, w_q, preferred_element_type=jnp.float32)
    proj_kv = jnp.dot(normed, w_kv, preferred_element_type=jnp.float32)
    position = lengths.astype(jnp.float32)
    queries = rotate(proj_q.reshape(BATCH, KVH, GROUP, HD), position[:, None, None]).astype(jnp.bfloat16)
    kv_parts = proj_kv.reshape(BATCH, 2, KVH, HD)
    new_keys = rotate(kv_parts[:, 0], position[:, None]).astype(jnp.bfloat16)
    new_values = kv_parts[:, 1].astype(jnp.bfloat16)
    visible = jnp.arange(CTX, dtype=jnp.int32)[None, :] < lengths[:, None]
    score_scale = 1.0 / HD ** 0.5

    def attend_head(kv_head):
        cache_head = kv_cache[kv_head][slab_index[kv_head]]
        key_cache = cache_head[:, 0].astype(jnp.float32)
        value_cache = cache_head[:, 1].astype(jnp.float32)
        head_queries = queries[:, kv_head].astype(jnp.float32)
        scores = jnp.einsum('bgd,bpd->bgp', head_queries, key_cache) * score_scale
        new_score = jnp.einsum('bgd,bd->bg', head_queries, new_keys[:, kv_head].astype(jnp.float32)) * score_scale
        row_max = jnp.maximum(lax.optimization_barrier(jnp.max(jnp.where(visible[:, None, :], scores, -1e+30), axis=2)), new_score)
        weights = jnp.where(visible[:, None, :], jnp.exp(scores - row_max[..., None]), 0.0)
        new_weight = jnp.exp(new_score - row_max)
        denominator = lax.optimization_barrier(jnp.sum(weights, axis=2)) + new_weight
        weighted = jnp.einsum('bgp,bpd->bgd', weights.astype(jnp.bfloat16).astype(jnp.float32), value_cache)
        weighted = weighted + new_weight.astype(jnp.bfloat16).astype(jnp.float32)[..., None] * new_values[:, kv_head].astype(jnp.float32)[:, None, :]
        return (weighted / denominator[..., None]).astype(jnp.bfloat16)
    heads_out = lax.map(attend_head, jnp.arange(KVH, dtype=jnp.int32))
    attention = jnp.transpose(heads_out, (1, 0, 2, 3)).reshape(BATCH, D)
    result = stream + jnp.dot(attention, w_o, preferred_element_type=jnp.float32)
    return result.astype(jnp.bfloat16)
```

```python
import functools

import jax
import jax.numpy as jnp
from jax import lax
from jax.experimental import pallas as pl
from jax.experimental.pallas import tpu as pltpu
from jax.sharding import PartitionSpec as P

KVH = 8
HD = 128
GROUP = 16

epsilon = 1e-05
rope_base = 500000.0
score_scale = 1.0 / HD**0.5
lowest = -1e30


def step_kernel(
    n,
    slab_ref,
    len_ref,
    hidden_ref,
    gain_ref,
    cos_ref,
    sin_ref,
    wq_hbm,
    wkv_hbm,
    wo_hbm,
    kv_hbm,
    out_ref,
    wq_v,
    wkv_v,
    wo_v,
    kv_v,
    sq_buf,
    kvp,
    part_buf,
    part_in,
    q_buf,
    fin,
    k_rows,
    v_rows,
    o_buf,
    o_in,
    st_buf,
    st_in,
    att_f,
    att_buf,
    wq_sem,
    wkv_sem,
    wo_sem,
    kv_sem,
    send_sem,
    recv_sem,
    att_sem,
):
    me = lax.axis_index("tensor")
    requests, width = hidden_ref.shape
    heads = KVH * GROUP // n
    cols = heads * HD
    q_rows = heads * requests
    per_kv = GROUP // heads
    slabs, positions = kv_v.shape[1], kv_v.shape[3]

    def wq_copy(step):
        owner = lax.rem(me + 1 + step, n)
        return pltpu.make_async_copy(
            wq_hbm.at[:, pl.ds(pl.multiple_of(owner * cols, cols), cols)],
            wq_v.at[step],
            wq_sem.at[step],
        )

    wkv_copy = pltpu.make_async_copy(wkv_hbm, wkv_v, wkv_sem)
    wo_copy = pltpu.make_async_copy(wo_hbm, wo_v, wo_sem)
    kv_copy = pltpu.make_async_copy(kv_hbm, kv_v, kv_sem)
    wkv_copy.start()

    @pl.loop(0, n)
    def _(step):
        wq_copy(step).start()

    def remote(src, dst, phase, peer):
        return pltpu.make_async_remote_copy(
            src_ref=src,
            dst_ref=dst,
            send_sem=send_sem.at[phase],
            recv_sem=recv_sem.at[phase],
            device_id={"tensor": peer},
            device_id_type=pl.DeviceIdType.MESH,
        )

    def wait_all(buf, phase, sent=True, received=True):
        every = buf.at[pl.ds(0, n - 1)]
        descriptor = remote(every, every, phase, lax.rem(me + 1, n))
        if received:
            descriptor.wait_recv()
        if sent:
            descriptor.wait_send()

    barrier = pltpu.get_barrier_semaphore()

    @pl.loop(1, n)
    def _(step):
        pl.semaphore_signal(
            barrier,
            inc=1,
            device_id={"tensor": lax.rem(me + step, n)},
            device_id_type=pl.DeviceIdType.MESH,
        )

    stream = hidden_ref[...].astype(jnp.float32)
    own_sq = jnp.sum(stream * stream, axis=1, keepdims=True)
    sq_buf[me] = jnp.broadcast_to(own_sq, (requests, HD))
    pl.semaphore_wait(barrier, n - 1)

    @pl.loop(1, n)
    def _(step):
        remote(sq_buf.at[me], sq_buf.at[me], 0, lax.rem(me + step, n)).start()

    wait_all(sq_buf, 0)
    squares = jnp.sum(sq_buf[...], axis=0)[:, :1]
    normed = (
        stream
        * lax.rsqrt(squares / (width * n) + epsilon)
        * gain_ref[...].astype(jnp.float32)
    ).astype(jnp.bfloat16)

    wkv_copy.wait()
    for piece in range(2 * KVH * HD // 512):
        res = jnp.dot(
            normed, wkv_v[:, piece * 512 : (piece + 1) * 512], preferred_element_type=jnp.float32
        )
        for j in range(4):
            kvp[piece * 4 + j] = res[:, j * HD : (j + 1) * HD]

    def project(step, target):
        owner = lax.rem(me + 1 + step, n)
        wq_copy(step).wait()
        res = jnp.dot(normed, wq_v[step], preferred_element_type=jnp.float32)
        for j in range(heads):
            target[j * requests : (j + 1) * requests, :] = res[:, j * HD : (j + 1) * HD]
        kv_head = owner // per_kv
        target[q_rows : q_rows + requests, :] = kvp[kv_head]
        target[q_rows + requests : q_rows + 2 * requests, :] = kvp[KVH + kv_head]
        return owner

    @pl.loop(0, n - 1)
    def _(step):
        owner = project(step, part_buf.at[step])
        remote(part_buf.at[step], part_in.at[me], 1, owner).start()

    kv_copy.start()
    wo_copy.start()
    project(n - 1, part_in.at[me])
    wait_all(part_in, 1)

    total = jnp.sum(part_in[...], axis=0)
    total = total * cos_ref[...] + pltpu.roll(total, HD // 2, 1) * sin_ref[...]
    rounded = total.astype(jnp.bfloat16)
    fin[...] = rounded.astype(jnp.float32)
    q_buf[me] = fin[:q_rows, :].astype(jnp.bfloat16)

    @pl.loop(1, n)
    def _(step):
        remote(q_buf.at[me], q_buf.at[me], 2, lax.rem(me + step, n)).start()

    for j in range(heads):
        k_rows[j * requests : (j + 1) * requests, :] = fin[q_rows : q_rows + requests, :]
        v_rows[j * requests : (j + 1) * requests, :] = fin[
            q_rows + requests : q_rows + 2 * requests, :
        ]
    new_score = jnp.sum(fin[:q_rows, :] * k_rows[...], axis=1, keepdims=True) * score_scale
    lane = lax.broadcasted_iota(jnp.int32, (q_rows, HD), 1)
    row = lax.broadcasted_iota(jnp.int32, (q_rows, HD), 0)
    diagonal = lane == row
    shifted = lane == row + HD // 2
    new_lane = jnp.sum(jnp.where(diagonal, new_score, 0.0), axis=0, keepdims=True)

    all_rows = GROUP * requests
    keys = slabs * positions
    row_req = lax.rem(lax.broadcasted_iota(jnp.int32, (all_rows, 1), 0), requests)
    column = lax.broadcasted_iota(jnp.int32, (1, keys), 1)
    column_slab = column // positions
    column_pos = lax.rem(column, positions) + me * positions
    row_len = jnp.zeros((all_rows, 1), jnp.int32)
    for b in range(requests):
        row_len = jnp.where(row_req == b, len_ref[b], row_len)
    in_length = column_pos < row_len

    kv_copy.wait()
    wait_all(q_buf, 2)

    @pl.loop(0, KVH)
    def _(h):
        row_slab = jnp.zeros((all_rows, 1), jnp.int32)
        for b in range(requests):
            row_slab = jnp.where(row_req == b, slab_ref[h, b], row_slab)
        visible = jnp.logical_and(column_slab == row_slab, in_length)
        queries = q_buf[pl.ds(h * per_kv, per_kv)].reshape(all_rows, HD)
        key_block = kv_v[h, :, 0].reshape(keys, HD)
        value_block = kv_v[h, :, 1].reshape(keys, HD)
        scores = (
            lax.dot_general(
                queries, key_block, (((1,), (1,)), ((), ())), preferred_element_type=jnp.float32
            )
            * score_scale
        )
        scores = jnp.where(visible, scores, lowest)
        top = jnp.max(scores, axis=1, keepdims=True)
        weights = jnp.where(visible, jnp.exp(scores - top), 0.0)
        weight_sum = jnp.sum(weights, axis=1, keepdims=True)
        weighted = jnp.dot(
            weights.astype(jnp.bfloat16), value_block, preferred_element_type=jnp.float32
        )
        for t in range(per_kv):
            owner = h * per_kv + t
            own = slice(t * q_rows, (t + 1) * q_rows)
            o_buf[owner] = weighted[own].astype(jnp.bfloat16)
            st_buf[owner] = jnp.sum(
                jnp.where(diagonal, top[own], 0.0) + jnp.where(shifted, weight_sum[own], 0.0),
                axis=0,
                keepdims=True,
            )

    o_in[me] = o_buf[me]
    st_in[me] = st_buf[me]

    @pl.loop(1, n)
    def _(step):
        peer = lax.rem(me + step, n)
        remote(st_buf.at[peer], st_in.at[me], 3, peer).start()
        remote(o_buf.at[peer], o_in.at[me], 4, peer).start()

    wait_all(st_in, 3)
    stats = st_in[...]
    top_lane = jnp.maximum(jnp.max(stats, axis=0), new_lane)
    factor = jnp.exp(jnp.minimum(stats - top_lane[None], 0.0))
    new_factor = jnp.exp(new_lane - top_lane)
    sums = jnp.concatenate([stats[:, :, HD // 2 :], stats[:, :, : HD // 2]], axis=2)
    denominator_lane = jnp.sum(factor * sums, axis=0) + new_factor

    def as_column(lanes):
        return jnp.sum(jnp.where(diagonal, lanes, 0.0), axis=1, keepdims=True)

    wait_all(o_in, 4)
    weighted = as_column(new_factor).astype(jnp.bfloat16).astype(jnp.float32) * v_rows[...]
    columns = jnp.sum(jnp.where(diagonal[None], factor, 0.0), axis=2, keepdims=True)
    weighted = weighted + jnp.sum(columns * o_in[...].astype(jnp.float32), axis=0)
    att_f[...] = weighted / as_column(denominator_lane)
    for j in range(heads):
        att_buf[me, :, j * HD : (j + 1) * HD] = att_f[
            j * requests : (j + 1) * requests, :
        ].astype(jnp.bfloat16)

    def att_copy(peer, source):
        return pltpu.make_async_remote_copy(
            src_ref=att_buf.at[source],
            dst_ref=att_buf.at[source],
            send_sem=send_sem.at[5],
            recv_sem=att_sem.at[source],
            device_id={"tensor": peer},
            device_id_type=pl.DeviceIdType.MESH,
        )

    @pl.loop(1, n)
    def _(step):
        att_copy(lax.rem(me + step, n), me).start()

    wo_copy.wait()

    def project_out(source):
        return jnp.dot(
            att_buf[source],
            wo_v[pl.ds(pl.multiple_of(source * cols, cols), cols), :],
            preferred_element_type=jnp.float32,
        )

    def add(step, acc):
        source = lax.rem(me + n - step, n)
        att_copy(lax.rem(me + 1, n), source).wait_recv()
        return acc + project_out(source)

    acc = lax.fori_loop(1, n, add, project_out(me))
    out_ref[...] = (stream + acc).astype(jnp.bfloat16)
    wait_all(att_buf, 5, received=False)


def body(n, hidden_in, norm_gain, w_q, w_kv, w_o, kv_cache, lengths, slab_index):
    requests, width = hidden_in.shape
    heads = KVH * GROUP // n
    cols = heads * HD
    q_rows = heads * requests
    all_rows = q_rows + 2 * requests
    slabs, positions = kv_cache.shape[1], kv_cache.shape[3]

    half = HD // 2
    frequency = rope_base ** (-2.0 * jnp.arange(half, dtype=jnp.float32) / HD)
    angles = lengths.astype(jnp.float32)[:, None] * frequency
    cosine, sine = jnp.cos(angles), jnp.sin(angles)
    cosine = jnp.concatenate([cosine, cosine], axis=1)
    sine = jnp.concatenate([-sine, sine], axis=1)
    cosine = jnp.concatenate([jnp.tile(cosine, (heads + 1, 1)), jnp.ones_like(cosine)], axis=0)
    sine = jnp.concatenate([jnp.tile(sine, (heads + 1, 1)), jnp.zeros_like(sine)], axis=0)

    vmem = pl.BlockSpec(memory_space=pltpu.VMEM)
    smem = pl.BlockSpec(memory_space=pltpu.SMEM)
    hbm = pl.BlockSpec(memory_space=pl.ANY)
    bf16, f32 = jnp.bfloat16, jnp.float32
    return pl.pallas_call(
        functools.partial(step_kernel, n),
        out_shape=jax.ShapeDtypeStruct((requests, width), bf16),
        in_specs=[smem, smem, vmem, vmem, vmem, vmem, hbm, hbm, hbm, hbm],
        out_specs=vmem,
        scratch_shapes=[
            pltpu.VMEM((n, width, cols), bf16),
            pltpu.VMEM(w_kv.shape, bf16),
            pltpu.VMEM(w_o.shape, bf16),
            pltpu.VMEM(kv_cache.shape, bf16),
            pltpu.VMEM((n, requests, HD), f32),
            pltpu.VMEM((2 * KVH, requests, HD), f32),
            pltpu.VMEM((n - 1, all_rows, HD), f32),
            pltpu.VMEM((n, all_rows, HD), f32),
            pltpu.VMEM((n, q_rows, HD), bf16),
            pltpu.VMEM((all_rows, HD), f32),
            pltpu.VMEM((q_rows, HD), f32),
            pltpu.VMEM((q_rows, HD), f32),
            pltpu.VMEM((n, q_rows, HD), bf16),
            pltpu.VMEM((n, q_rows, HD), bf16),
            pltpu.VMEM((n, 1, HD), f32),
            pltpu.VMEM((n, 1, HD), f32),
            pltpu.VMEM((q_rows, HD), f32),
            pltpu.VMEM((n, requests, cols), bf16),
            pltpu.SemaphoreType.DMA((n,)),
            pltpu.SemaphoreType.DMA,
            pltpu.SemaphoreType.DMA,
            pltpu.SemaphoreType.DMA,
            pltpu.SemaphoreType.DMA((6,)),
            pltpu.SemaphoreType.DMA((5,)),
            pltpu.SemaphoreType.DMA((n,)),
        ],
        compiler_params=pltpu.CompilerParams(
            collective_id=0, has_side_effects=True, vmem_limit_bytes=56 * 1024 * 1024
        ),
    )(
        slab_index,
        lengths,
        hidden_in,
        norm_gain.reshape(1, width),
        cosine,
        sine,
        w_q,
        w_kv,
        w_o,
        kv_cache,
    )


def solution(mesh):
    placed = (
        P("groups", "tensor"),
        P("tensor"),
        P("tensor", None),
        P("tensor", None),
        P(None, "tensor"),
        P(None, "groups", None, "tensor", None),
        P("groups"),
        P(None, "groups"),
    )
    return jax.shard_map(
        functools.partial(body, mesh.shape["tensor"]),
        mesh=mesh,
        in_specs=placed,
        out_specs=P("groups", "tensor"),
        check_vma=False,
    )
```

```python
import functools

import jax
import jax.numpy as jnp
from jax import lax
from jax.experimental import pallas as pl
from jax.experimental.pallas import tpu as pltpu
from jax.sharding import PartitionSpec as P

KVH = 8
HD = 128
GROUP = 16

epsilon = 1e-05
rope_base = 500000.0
score_scale = 1.0 / HD**0.5
lowest = -1e30


def step_kernel(
    n,
    slab_ref,
    len_ref,
    hidden_ref,
    gain_ref,
    cos_ref,
    sin_ref,
    wq_hbm,
    wkv_hbm,
    wo_hbm,
    kv_hbm,
    out_ref,
    wq_v,
    wkv_v,
    wo_v,
    kv_v,
    sq_buf,
    kvp,
    part_buf,
    part_in,
    q_buf,
    fin,
    k_rows,
    v_rows,
    o_buf,
    o_in,
    st_buf,
    st_in,
    att_f,
    att_buf,
    wq_sem,
    wkv_sem,
    wo_sem,
    kv_sem,
    send_sem,
    recv_sem,
    att_sem,
):
    me = lax.axis_index("tensor")
    requests, width = hidden_ref.shape
    heads = KVH * GROUP // n
    cols = heads * HD
    q_rows = heads * requests
    per_kv = GROUP // heads
    slabs, positions = kv_v.shape[1], kv_v.shape[3]

    def wq_copy(step):
        owner = lax.rem(me + 1 + step, n)
        return pltpu.make_async_copy(
            wq_hbm.at[:, pl.ds(pl.multiple_of(owner * cols, cols), cols)],
            wq_v.at[step],
            wq_sem.at[step],
        )

    wkv_copy = pltpu.make_async_copy(wkv_hbm, wkv_v, wkv_sem)
    wo_copy = pltpu.make_async_copy(wo_hbm, wo_v, wo_sem)
    kv_copy = pltpu.make_async_copy(kv_hbm, kv_v, kv_sem)
    wkv_copy.start()

    @pl.loop(0, n)
    def _(step):
        wq_copy(step).start()

    def remote(src, dst, phase, peer):
        return pltpu.make_async_remote_copy(
            src_ref=src,
            dst_ref=dst,
            send_sem=send_sem.at[phase],
            recv_sem=recv_sem.at[phase],
            device_id={"tensor": peer},
            device_id_type=pl.DeviceIdType.MESH,
        )

    def wait_all(buf, phase, sent=True, received=True):
        every = buf.at[pl.ds(0, n - 1)]
        descriptor = remote(every, every, phase, lax.rem(me + 1, n))
        if received:
            descriptor.wait_recv()
        if sent:
            descriptor.wait_send()

    barrier = pltpu.get_barrier_semaphore()

    @pl.loop(1, n)
    def _(step):
        pl.semaphore_signal(
            barrier,
            inc=1,
            device_id={"tensor": lax.rem(me + step, n)},
            device_id_type=pl.DeviceIdType.MESH,
        )

    stream = hidden_ref[...].astype(jnp.float32)
    own_sq = jnp.sum(stream * stream, axis=1, keepdims=True)
    sq_buf[me] = jnp.broadcast_to(own_sq, (requests, HD))
    pl.semaphore_wait(barrier, n - 1)

    @pl.loop(1, n)
    def _(step):
        remote(sq_buf.at[me], sq_buf.at[me], 0, lax.rem(me + step, n)).start()

    wait_all(sq_buf, 0)
    squares = jnp.sum(sq_buf[...], axis=0)[:, :1]
    normed = (
        stream
        * lax.rsqrt(squares / (width * n) + epsilon)
        * gain_ref[...].astype(jnp.float32)
    ).astype(jnp.bfloat16)

    wkv_copy.wait()
    for piece in range(2 * KVH * HD // 512):
        res = jnp.dot(
            normed, wkv_v[:, piece * 512 : (piece + 1) * 512], preferred_element_type=jnp.float32
        )
        for j in range(4):
            kvp[piece * 4 + j] = res[:, j * HD : (j + 1) * HD]

    def project(step, target):
        owner = lax.rem(me + 1 + step, n)
        wq_copy(step).wait()
        res = jnp.dot(normed, wq_v[step], preferred_element_type=jnp.float32)
        for j in range(heads):
            target[j * requests : (j + 1) * requests, :] = res[:, j * HD : (j + 1) * HD]
        kv_head = owner // per_kv
        target[q_rows : q_rows + requests, :] = kvp[kv_head]
        target[q_rows + requests : q_rows + 2 * requests, :] = kvp[KVH + kv_head]
        return owner

    @pl.loop(0, n - 1, unroll=True)
    def _(step):
        owner = project(step, part_buf.at[step])
        remote(part_buf.at[step], part_in.at[me], 1, owner).start()

    kv_copy.start()
    wo_copy.start()
    project(n - 1, part_in.at[me])
    wait_all(part_in, 1)

    total = jnp.sum(part_in[...], axis=0)
    total = total * cos_ref[...] + pltpu.roll(total, HD // 2, 1) * sin_ref[...]
    rounded = total.astype(jnp.bfloat16)
    fin[...] = rounded.astype(jnp.float32)
    q_buf[me] = fin[:q_rows, :].astype(jnp.bfloat16)

    @pl.loop(1, n)
    def _(step):
        remote(q_buf.at[me], q_buf.at[me], 2, lax.rem(me + step, n)).start()

    for j in range(heads):
        k_rows[j * requests : (j + 1) * requests, :] = fin[q_rows : q_rows + requests, :]
        v_rows[j * requests : (j + 1) * requests, :] = fin[
            q_rows + requests : q_rows + 2 * requests, :
        ]
    new_score = jnp.sum(fin[:q_rows, :] * k_rows[...], axis=1, keepdims=True) * score_scale
    lane = lax.broadcasted_iota(jnp.int32, (q_rows, HD), 1)
    row = lax.broadcasted_iota(jnp.int32, (q_rows, HD), 0)
    diagonal = lane == row
    shifted = lane == row + HD // 2
    new_lane = jnp.sum(jnp.where(diagonal, new_score, 0.0), axis=0, keepdims=True)

    all_rows = GROUP * requests
    keys = slabs * positions
    row_req = lax.rem(lax.broadcasted_iota(jnp.int32, (all_rows, 1), 0), requests)
    column = lax.broadcasted_iota(jnp.int32, (1, keys), 1)
    column_slab = column // positions
    column_pos = lax.rem(column, positions) + me * positions
    row_len = jnp.zeros((all_rows, 1), jnp.int32)
    for b in range(requests):
        row_len = jnp.where(row_req == b, len_ref[b], row_len)
    in_length = column_pos < row_len

    kv_copy.wait()
    wait_all(q_buf, 2)

    @pl.loop(0, KVH, unroll=True)
    def _(h):
        row_slab = jnp.zeros((all_rows, 1), jnp.int32)
        for b in range(requests):
            row_slab = jnp.where(row_req == b, slab_ref[h, b], row_slab)
        visible = jnp.logical_and(column_slab == row_slab, in_length)
        queries = q_buf[pl.ds(h * per_kv, per_kv)].reshape(all_rows, HD)
        key_block = kv_v[h, :, 0].reshape(keys, HD)
        value_block = kv_v[h, :, 1].reshape(keys, HD)
        scores = (
            lax.dot_general(
                queries, key_block, (((1,), (1,)), ((), ())), preferred_element_type=jnp.float32
            )
            * score_scale
        )
        scores = jnp.where(visible, scores, lowest)
        top = jnp.max(scores, axis=1, keepdims=True)
        weights = jnp.where(visible, jnp.exp(scores - top), 0.0)
        weight_sum = jnp.sum(weights, axis=1, keepdims=True)
        weighted = jnp.dot(
            weights.astype(jnp.bfloat16), value_block, preferred_element_type=jnp.float32
        )
        for t in range(per_kv):
            owner = h * per_kv + t
            own = slice(t * q_rows, (t + 1) * q_rows)
            o_buf[owner] = weighted[own].astype(jnp.bfloat16)
            st_buf[owner] = jnp.sum(
                jnp.where(diagonal, top[own], 0.0) + jnp.where(shifted, weight_sum[own], 0.0),
                axis=0,
                keepdims=True,
            )

    o_in[me] = o_buf[me]
    st_in[me] = st_buf[me]

    @pl.loop(1, n)
    def _(step):
        peer = lax.rem(me + step, n)
        remote(st_buf.at[peer], st_in.at[me], 3, peer).start()
        remote(o_buf.at[peer], o_in.at[me], 4, peer).start()

    wait_all(st_in, 3)
    stats = st_in[...]
    top_lane = jnp.maximum(jnp.max(stats, axis=0), new_lane)
    factor = jnp.exp(jnp.minimum(stats - top_lane[None], 0.0))
    new_factor = jnp.exp(new_lane - top_lane)
    sums = jnp.concatenate([stats[:, :, HD // 2 :], stats[:, :, : HD // 2]], axis=2)
    denominator_lane = jnp.sum(factor * sums, axis=0) + new_factor

    def as_column(lanes):
        return jnp.sum(jnp.where(diagonal, lanes, 0.0), axis=1, keepdims=True)

    wait_all(o_in, 4)
    weighted = as_column(new_factor).astype(jnp.bfloat16).astype(jnp.float32) * v_rows[...]
    columns = jnp.sum(jnp.where(diagonal[None], factor, 0.0), axis=2, keepdims=True)
    weighted = weighted + jnp.sum(columns * o_in[...].astype(jnp.float32), axis=0)
    att_f[...] = weighted / as_column(denominator_lane)
    for j in range(heads):
        att_buf[me, :, j * HD : (j + 1) * HD] = att_f[
            j * requests : (j + 1) * requests, :
        ].astype(jnp.bfloat16)

    def att_copy(peer, source):
        return pltpu.make_async_remote_copy(
            src_ref=att_buf.at[source],
            dst_ref=att_buf.at[source],
            send_sem=send_sem.at[5],
            recv_sem=att_sem.at[source],
            device_id={"tensor": peer},
            device_id_type=pl.DeviceIdType.MESH,
        )

    @pl.loop(1, n)
    def _(step):
        att_copy(lax.rem(me + step, n), me).start()

    wo_copy.wait()

    def project_out(source):
        return jnp.dot(
            att_buf[source],
            wo_v[pl.ds(pl.multiple_of(source * cols, cols), cols), :],
            preferred_element_type=jnp.float32,
        )

    def add(step, acc):
        source = lax.rem(me + n - step, n)
        att_copy(lax.rem(me + 1, n), source).wait_recv()
        return acc + project_out(source)

    acc = lax.fori_loop(1, n, add, project_out(me))
    out_ref[...] = (stream + acc).astype(jnp.bfloat16)
    wait_all(att_buf, 5, received=False)


def body(n, hidden_in, norm_gain, w_q, w_kv, w_o, kv_cache, lengths, slab_index):
    requests, width = hidden_in.shape
    heads = KVH * GROUP // n
    cols = heads * HD
    q_rows = heads * requests
    all_rows = q_rows + 2 * requests
    slabs, positions = kv_cache.shape[1], kv_cache.shape[3]

    half = HD // 2
    frequency = rope_base ** (-2.0 * jnp.arange(half, dtype=jnp.float32) / HD)
    angles = lengths.astype(jnp.float32)[:, None] * frequency
    cosine, sine = jnp.cos(angles), jnp.sin(angles)
    cosine = jnp.concatenate([cosine, cosine], axis=1)
    sine = jnp.concatenate([-sine, sine], axis=1)
    cosine = jnp.concatenate([jnp.tile(cosine, (heads + 1, 1)), jnp.ones_like(cosine)], axis=0)
    sine = jnp.concatenate([jnp.tile(sine, (heads + 1, 1)), jnp.zeros_like(sine)], axis=0)

    vmem = pl.BlockSpec(memory_space=pltpu.VMEM)
    smem = pl.BlockSpec(memory_space=pltpu.SMEM)
    hbm = pl.BlockSpec(memory_space=pl.ANY)
    bf16, f32 = jnp.bfloat16, jnp.float32
    return pl.pallas_call(
        functools.partial(step_kernel, n),
        out_shape=jax.ShapeDtypeStruct((requests, width), bf16),
        in_specs=[smem, smem, vmem, vmem, vmem, vmem, hbm, hbm, hbm, hbm],
        out_specs=vmem,
        scratch_shapes=[
            pltpu.VMEM((n, width, cols), bf16),
            pltpu.VMEM(w_kv.shape, bf16),
            pltpu.VMEM(w_o.shape, bf16),
            pltpu.VMEM(kv_cache.shape, bf16),
            pltpu.VMEM((n, requests, HD), f32),
            pltpu.VMEM((2 * KVH, requests, HD), f32),
            pltpu.VMEM((n - 1, all_rows, HD), f32),
            pltpu.VMEM((n, all_rows, HD), f32),
            pltpu.VMEM((n, q_rows, HD), bf16),
            pltpu.VMEM((all_rows, HD), f32),
            pltpu.VMEM((q_rows, HD), f32),
            pltpu.VMEM((q_rows, HD), f32),
            pltpu.VMEM((n, q_rows, HD), bf16),
            pltpu.VMEM((n, q_rows, HD), bf16),
            pltpu.VMEM((n, 1, HD), f32),
            pltpu.VMEM((n, 1, HD), f32),
            pltpu.VMEM((q_rows, HD), f32),
            pltpu.VMEM((n, requests, cols), bf16),
            pltpu.SemaphoreType.DMA((n,)),
            pltpu.SemaphoreType.DMA,
            pltpu.SemaphoreType.DMA,
            pltpu.SemaphoreType.DMA,
            pltpu.SemaphoreType.DMA((6,)),
            pltpu.SemaphoreType.DMA((5,)),
            pltpu.SemaphoreType.DMA((n,)),
        ],
        compiler_params=pltpu.CompilerParams(
            collective_id=0, has_side_effects=True, vmem_limit_bytes=56 * 1024 * 1024
        ),
    )(
        slab_index,
        lengths,
        hidden_in,
        norm_gain.reshape(1, width),
        cosine,
        sine,
        w_q,
        w_kv,
        w_o,
        kv_cache,
    )


def solution(mesh):
    placed = (
        P("groups", "tensor"),
        P("tensor"),
        P("tensor", None),
        P("tensor", None),
        P(None, "tensor"),
        P(None, "groups", None, "tensor", None),
        P("groups"),
        P(None, "groups"),
    )
    return jax.shard_map(
        functools.partial(body, mesh.shape["tensor"]),
        mesh=mesh,
        in_specs=placed,
        out_specs=P("groups", "tensor"),
        check_vma=False,
    )
```
